32 devices in a mesh: fsdp: 8 (over z, core), chan: 4 (over y, x).
Axes of the slice: x: 2, y: 2, z: 4, core: 2. Of those that a mesh axis runs over, the one named last changes fastest.
Arguments:
- in_master: float32 [4096, 2, 4096], P(('fsdp', 'chan')), may hold values from -0.09375 to 0.09375
- in_moment: float32 [4096, 2, 4096], P(('fsdp', 'chan')), may hold values from -1.8 to 1.8
- in_velocity: float32 [4096, 2, 4096], P(('fsdp', 'chan')), may hold values from 0.05 to 1
- in_grad: bfloat16 [4096, 2, 4096], P(('fsdp', 'chan')), may hold values from -6 to 6
- out_master: float32 [4096, 4096], P(('fsdp', 'chan')), may hold values from -0.09375 to 0.09375
- out_moment: float32 [4096, 4096], P(('fsdp', 'chan')), may hold values from -1.8 to 1.8
- out_velocity: float32 [4096, 4096], P(('fsdp', 'chan')), may hold values from 0.001 to 1
- out_grad: bfloat16 [4096, 4096], P(('fsdp', 'chan')), may hold values from -6 to 6
- embed_table: bfloat16 [65536, 4096], P('fsdp', 'chan'), may hold values from -18 to 18
- tokens: int32 [4, 1024], P(None, 'fsdp'), may hold values from 0 to 65535, as said below
- conv_state: bfloat16 [1024, 3, 4096], P('fsdp', None, 'chan'), may hold values from -6 to 6
- ssm_state: float32 [1024, 16, 4096], P('fsdp', None, 'chan'), may hold values from -6 to 6
- conv_weight: float32 [4, 4096], P(None, 'chan'), may hold values from -3 to 3
- conv_bias: float32 [4096], P('chan'), may hold values from -3 to 3
- x_proj_w: bfloat16 [288, 4096], P(None, 'chan'), may hold values from -0.09375 to 0.09375
- dt_proj_w: bfloat16 [4096, 256], P('chan'), may hold values from -0.375 to 0.375
- dt_bias: float32 [4096], P('chan'), may hold values from -4.5 to -2
- a_log: float32 [16, 4096], P(None, 'chan'), may hold values from 0 to 2.77
- d_skip: float32 [4096], P('chan'), may hold values from 0.5 to 2
Outputs:
- in_master_new: float32 [4096, 2, 4096], P(('fsdp', 'chan'))
- out_master_new: float32 [4096, 4096], P(('fsdp', 'chan'))
- block_out: bfloat16 [4, 1024, 4096], P(None, 'fsdp', 'chan')
- conv_state_new: bfloat16 [1024, 3, 4096], P('fsdp', None, 'chan')
- ssm_state_new: float32 [1024, 16, 4096], P('fsdp', None, 'chan')
The draws below stay inside these ranges and needn't reach their ends.
Inputs may be any that keep to these rules, and one draw needn't show every extreme that they name: Split the ids into 8 equal consecutive vocabulary blocks and the sequences into 8 equal consecutive replicas; of one replica's 4 x 128 tokens at most 128 lie in any one block, and some block holds exactly 128 of them.
All inputs are finite; a program needn't handle non-finite values.
Results may differ from the reference program's by a relative error of at most 0.012.
Values may be sent and summed in bfloat16 or wider, within the bound.
A program may use at most 192 MiB of HBM per device.

```python
import math
import jax
import jax.numpy as jnp
from jax import lax

D = 4096
DI = 4096
RANK = 256
NSTATE = 16
KERNEL = 4
VOCAB = 65536
STEPS = 4
ROWS = 128
ALLROWS = 1024
CAP = 128
N_CHAN = 4


def draw_embed_table(key, part):
    keys = jax.random.split(jax.random.fold_in(key, 17), 3)
    row_scale = jnp.exp(jax.random.uniform(keys[0], (VOCAB, 1), jnp.float32, math.log(0.2), math.log(2.0)))
    col_scale = jnp.exp(jax.random.uniform(keys[1], (1, D), jnp.float32, math.log(0.3), math.log(3.0)))
    base = jnp.clip(jax.random.normal(keys[2], (VOCAB, D), jnp.float32), -3.0, 3.0)
    return (base * row_scale * col_scale).astype(jnp.bfloat16)


def draw_tokens(key, part):
    base = jax.random.fold_in(key, 29)
    replicas = ALLROWS // ROWS
    count = STEPS * ROWS
    block_ids = VOCAB // replicas
    slots = replicas * CAP

    def one_replica(inner_key):
        keys = jax.random.split(inner_key, 4)
        scores = jax.random.permutation(keys[0], slots).astype(jnp.int32)
        full_block = jax.random.randint(keys[1], (), 0, replicas, jnp.int32)
        slot_block = (jnp.arange(slots, dtype=jnp.int32) // CAP).astype(jnp.int32)
        scores = jnp.where(slot_block == full_block, scores - slots, scores)
        chosen = jnp.argsort(scores, stable=True)[:count].astype(jnp.int32)
        chosen = jax.random.permutation(keys[2], chosen)
        owner = chosen // CAP
        within = jax.random.randint(keys[3], (count,), 0, block_ids, jnp.int32)
        return (owner * block_ids + within).astype(jnp.int32)
    every = jax.vmap(one_replica)(jax.random.split(base, replicas))
    return jnp.transpose(every.reshape(replicas, STEPS, ROWS), (1, 0, 2)).reshape(STEPS, ALLROWS).astype(jnp.int32)


def steps_of(stream_key, extent, shards, low, top_value):
    def one(axis_at, shards_of):
        draws = jax.random.uniform(jax.random.fold_in(jax.random.fold_in(stream_key, 6), axis_at), (shards_of,), jnp.float32, low / len(shards), top_value / len(shards))
        return jnp.repeat(jnp.exp(draws), extent[axis_at] // shards_of).reshape((-1,) + (1,) * (len(extent) - axis_at - 1))

    level = one(*shards[0])
    for cut in shards[1:]:
        level = level * one(*cut)
    return level


def normal_values(key, extent, spread, bound, pieces=(), kind=jnp.bfloat16):
    entries = jax.random.normal(key, extent, jnp.float32) * spread
    if len(pieces) > 0:
        entries = steps_of(key, extent, pieces, -0.22, 0.18) * entries
    return jnp.clip(entries, min=-bound, max=bound).astype(kind)


def setup_inputs(seed: int = 0) -> dict:
    splits = jax.random.split(jax.random.key(seed), 20)
    in_master = normal_values(splits[0], (D, 2, DI), D ** -0.5, 0.09375, ((0, 32),), jnp.float32)
    in_moment = normal_values(splits[1], (D, 2, DI), 0.3, 1.8, ((0, 32),), jnp.float32)
    in_velocity = jnp.clip(jnp.exp(math.log(1.0) - 2.9957323 * jax.random.uniform(splits[2], (D, 2, DI), jnp.float32) ** steps_of(splits[2], (D, 2, DI), ((0, 32),), -0.2, 0.2)), 0.05, 1.0)
    in_grad = normal_values(splits[3], (D, 2, DI), 1.0, 6.0, ((0, 32),))
    out_master = normal_values(splits[4], (D, DI), DI ** -0.5, 0.09375, ((0, 32),), jnp.float32)
    out_moment = normal_values(splits[5], (D, DI), 0.3, 1.8, ((0, 32),), jnp.float32)
    out_velocity = jnp.clip(jnp.exp(math.log(1.0) - 6.9077552 * jax.random.uniform(splits[6], (D, DI), jnp.float32) ** steps_of(splits[6], (D, DI), ((0, 32),), -0.2, 0.2)), 0.001, 1.0)
    out_grad = normal_values(splits[7], (D, DI), 1.0, 6.0, ((0, 32),))
    embed_table = draw_embed_table(jax.random.fold_in(splits[19], 71), 0)
    tokens = draw_tokens(jax.random.fold_in(splits[19], 71), 0)
    conv_state = normal_values(splits[10], (ALLROWS, KERNEL - 1, DI), 1.0, 6.0, ((0, 8), (2, 4)))
    ssm_state = normal_values(splits[11], (ALLROWS, NSTATE, DI), 1.0, 6.0, ((0, 8), (2, 4)), jnp.float32)
    conv_weight = normal_values(splits[12], (KERNEL, DI), KERNEL ** -0.5, 3.0, ((1, 4),), jnp.float32)
    conv_bias = normal_values(splits[13], (DI,), 0.5, 3.0, ((0, 4),), jnp.float32)
    x_proj_w = normal_values(splits[14], (RANK + 2 * NSTATE, DI), DI ** -0.5, 0.09375, ((1, 4),))
    dt_proj_w = normal_values(splits[15], (DI, RANK), RANK ** -0.5, 0.375, ((0, 4),))
    dt_bias = jnp.clip(-4.5 + 2.5 * jax.random.uniform(splits[16], (DI,), jnp.float32) ** steps_of(splits[16], (DI,), ((0, 4),), -0.2, 0.2), -4.5, -2.0)
    a_log = jnp.clip(2.77 * jax.random.uniform(splits[17], (NSTATE, DI), jnp.float32) ** steps_of(splits[17], (NSTATE, DI), ((1, 4),), -0.2, 0.2), 0.0, 2.77)
    d_skip = jnp.clip(0.5 + 1.5 * jax.random.uniform(splits[18], (DI,), jnp.float32) ** steps_of(splits[18], (DI,), ((0, 4),), -0.2, 0.2), 0.5, 2.0)
    return {"in_master": in_master, "in_moment": in_moment, "in_velocity": in_velocity, "in_grad": in_grad, "out_master": out_master, "out_moment": out_moment, "out_velocity": out_velocity, "out_grad": out_grad, "embed_table": embed_table, "tokens": tokens, "conv_state": conv_state, "ssm_state": ssm_state, "conv_weight": conv_weight, "conv_bias": conv_bias, "x_proj_w": x_proj_w, "dt_proj_w": dt_proj_w, "dt_bias": dt_bias, "a_log": a_log, "d_skip": d_skip}


learn_rate = 0.01
beta_first = 0.8
beta_second = 0.95
adam_eps = 1e-08
weight_decay = 0.1
bias_first = 1.0 - math.pow(0.8, 10)
bias_second = 1.0 - math.pow(0.95, 10)
norm_eps = 1e-06

def adam_update(master, moment, velocity, grad):
    gradient = grad.astype(jnp.float32)
    moment = beta_first * moment + (1.0 - beta_first) * gradient
    velocity = beta_second * velocity + (1.0 - beta_second) * gradient * gradient
    update = moment / bias_first / (jnp.sqrt(velocity / bias_second) + adam_eps)
    return master - learn_rate * (update + weight_decay * master)

def reference(in_master, in_moment, in_velocity, in_grad, out_master, out_moment, out_velocity, out_grad, embed_table, tokens, conv_state, ssm_state, conv_weight, conv_bias, x_proj_w, dt_proj_w, dt_bias, a_log, d_skip):
    in_new = adam_update(in_master, in_moment, in_velocity, in_grad)
    out_new = adam_update(out_master, out_moment, out_velocity, out_grad)
    relay_x = in_new[:, 0, :].astype(jnp.bfloat16)
    relay_z = in_new[:, 1, :].astype(jnp.bfloat16)
    relay_out = out_new.astype(jnp.bfloat16)
    inputs = embed_table[tokens]
    steps, rows = tokens.shape
    flat = inputs.reshape(steps * rows, D).astype(jnp.float32)
    normed = (flat * lax.rsqrt(lax.optimization_barrier(jnp.mean(flat * flat, axis=1, keepdims=True)) + norm_eps)).astype(jnp.bfloat16)
    x_in = jnp.dot(normed, relay_x, preferred_element_type=jnp.float32).astype(jnp.bfloat16).reshape(steps, rows, DI)
    z_in = jnp.dot(normed, relay_z, preferred_element_type=jnp.float32).astype(jnp.bfloat16).reshape(steps, rows, DI)
    decay = -jnp.exp(a_log)
    group_width = DI // N_CHAN
    weight_groups = relay_out.reshape(D, N_CHAN, group_width).astype(jnp.float32)
    window_state = conv_state
    state = ssm_state
    outputs = []
    for step in range(steps):
        window = jnp.concatenate([window_state, x_in[step][:, None, :]], axis=1)
        mixed_conv = lax.optimization_barrier(jnp.sum(window.astype(jnp.float32) * conv_weight[None], axis=1)) + conv_bias
        act = jax.nn.silu(mixed_conv).astype(jnp.bfloat16)
        dbc = jnp.dot(act, x_proj_w.T, preferred_element_type=jnp.float32)
        dt_low = dbc[:, :RANK].astype(jnp.bfloat16)
        b_mat = dbc[:, RANK:RANK + NSTATE]
        c_mat = dbc[:, RANK + NSTATE:]
        delta = jax.nn.softplus(jnp.dot(dt_low, dt_proj_w.T, preferred_element_type=jnp.float32) + dt_bias)
        act_real = act.astype(jnp.float32)
        state = jnp.exp(delta[:, None, :] * decay[None]) * state + (delta * act_real)[:, None, :] * b_mat[:, :, None]
        y_out = lax.optimization_barrier(jnp.sum(c_mat[:, :, None] * state, axis=1)) + d_skip * act_real
        gated = (y_out * jax.nn.silu(z_in[step].astype(jnp.float32))).astype(jnp.bfloat16)
        gated_groups = gated.reshape(rows, N_CHAN, group_width).astype(jnp.float32)
        partials = jnp.einsum('rgk,dgk->grd', gated_groups, weight_groups, precision=lax.Precision.HIGHEST)
        partials = lax.optimization_barrier(partials.astype(jnp.bfloat16))
        mixed = lax.optimization_barrier(jnp.sum(partials.astype(jnp.float32), axis=0))
        outputs.append((inputs[step].astype(jnp.float32) + mixed).astype(jnp.bfloat16))
        window_state = window[:, 1:, :]
    return (in_new, out_new, jnp.stack(outputs), window_state, state)
```

```python
import math

import jax
import jax.numpy as jnp
from jax import lax
from jax.experimental.layout import Layout, with_layout_constraint
from jax.sharding import PartitionSpec as P

RANK = 256
NSTATE = 16


learn_rate = 0.01
beta_first = 0.8
beta_second = 0.95
adam_eps = 1e-08
weight_decay = 0.1
bias_first = 1.0 - math.pow(0.8, 10)
bias_second = 1.0 - math.pow(0.95, 10)
norm_eps = 1e-06


def adam_update(master, moment, velocity, grad):
    gradient = grad.astype(jnp.float32)
    moment = beta_first * moment + (1.0 - beta_first) * gradient
    velocity = beta_second * velocity + (1.0 - beta_second) * gradient * gradient
    update = moment / bias_first / (jnp.sqrt(velocity / bias_second) + adam_eps)
    return master - learn_rate * (update + weight_decay * master)


def row_major(block):
    return with_layout_constraint(block, Layout(tuple(range(block.ndim))))


def exchange(block, axis):
    return row_major(
        lax.all_to_all(row_major(block), axis, split_axis=0, concat_axis=0, tiled=True)
    )


def gather_by_exchange(block, axis):
    count = lax.axis_size(axis)
    spread = jnp.broadcast_to(block[None], (count,) + block.shape)
    return exchange(spread, axis)


def owned_rank(member):
    length = member.shape[0]
    earlier = lax.broadcasted_iota(jnp.int32, (length, length), 1) < lax.broadcasted_iota(
        jnp.int32, (length, length), 0
    )
    return jnp.dot(
        earlier.astype(jnp.bfloat16),
        member.astype(jnp.bfloat16),
        preferred_element_type=jnp.float32,
    ).astype(jnp.int32)


def find_inputs(embed_table, tokens):
    replicas = lax.axis_size("fsdp")
    vocab_rows = embed_table.shape[0]
    mine = tokens.reshape(-1)
    count = mine.shape[0]
    cap = 2 * count // replicas
    every = lax.all_gather(mine, "fsdp", axis=0, tiled=False)
    offset = every - lax.axis_index("fsdp") * vocab_rows
    inside = jnp.logical_and(offset >= 0, offset < vocab_rows)
    rank = owned_rank(inside.T).T
    key = jnp.where(inside, rank, -1)
    slot_ids = lax.broadcasted_iota(jnp.int32, (replicas, cap, count), 1)
    slots = jnp.sum(jnp.where(key[:, None, :] == slot_ids, offset[:, None, :], 0), axis=2)
    rows = embed_table.at[slots.reshape(-1)].get(mode="clip")
    got = exchange(rows, "fsdp")
    owner = mine // vocab_rows
    member = owner[:, None] == lax.broadcasted_iota(jnp.int32, (count, replicas), 1)
    place = owner * cap + jnp.sum(jnp.where(member, owned_rank(member), 0), axis=1)
    pick = place[:, None] == lax.broadcasted_iota(jnp.int32, (count, replicas * cap), 1)
    return jnp.dot(pick.astype(jnp.bfloat16), got, preferred_element_type=jnp.float32).astype(
        jnp.bfloat16
    )


def per_device(
    in_master,
    in_moment,
    in_velocity,
    in_grad,
    out_master,
    out_moment,
    out_velocity,
    out_grad,
    embed_table,
    tokens,
    conv_state,
    ssm_state,
    conv_weight,
    conv_bias,
    x_proj_w,
    dt_proj_w,
    dt_bias,
    a_log,
    d_skip,
):
    groups = lax.axis_size("chan")
    replicas = lax.axis_size("fsdp")
    steps, rows = tokens.shape
    in_new = adam_update(in_master, in_moment, in_velocity, in_grad)
    in_new = lax.optimization_barrier(row_major(in_new))
    out_new = adam_update(out_master, out_moment, out_velocity, out_grad)
    out_new = lax.optimization_barrier(row_major(out_new))
    x_piece = in_new[:, 0, :].astype(jnp.bfloat16)
    z_piece = in_new[:, 1, :].astype(jnp.bfloat16)
    out_piece = out_new.astype(jnp.bfloat16)

    def to_groups(piece):
        shaped = piece.reshape(piece.shape[0], groups, -1)
        split = jnp.transpose(shaped, (1, 0, 2))
        return exchange(split, "chan").reshape(-1, split.shape[2])

    x_own, z_own, out_own = to_groups(x_piece), to_groups(z_piece), to_groups(out_piece)
    relay_x = lax.all_gather(x_own, "fsdp", axis=0, tiled=True)
    relay_z = lax.all_gather(z_own, "fsdp", axis=0, tiled=True)
    half = out_own.shape[0] // 2
    relay_out = [
        lax.all_gather(out_own[at * half : (at + 1) * half], "fsdp", axis=0, tiled=True)
        for at in range(2)
    ]

    found = find_inputs(embed_table, tokens)
    parts = gather_by_exchange(found, "chan")
    flat = parts.astype(jnp.float32)
    width = groups * parts.shape[2]
    square = jnp.sum(jnp.sum(flat * flat, axis=2), axis=0) / width
    scale = lax.rsqrt(square + norm_eps)
    normed = (flat * scale[None, :, None]).astype(jnp.bfloat16)
    normed = jnp.transpose(normed, (1, 0, 2)).reshape(steps * rows, width)
    x_in = (
        jnp.dot(normed, relay_x, preferred_element_type=jnp.float32)
        .astype(jnp.bfloat16)
        .reshape(steps, rows, -1)
    )
    decay = -jnp.exp(a_log)
    contract_last = (((1,), (1,)), ((), ()))
    window = jnp.concatenate([jnp.transpose(conv_state, (1, 0, 2)), x_in], axis=0)
    taps = conv_weight.shape[0]
    acts = []
    for step in range(steps):
        total = conv_bias
        for tap in range(taps):
            total = total + window[step + tap].astype(jnp.float32) * conv_weight[tap]
        acts.append(jax.nn.silu(total).astype(jnp.bfloat16))
    act_all = jnp.concatenate(acts, axis=0)
    partial_value = lax.dot_general(
        act_all, x_proj_w, contract_last, preferred_element_type=jnp.float32
    )
    dbc = jnp.sum(gather_by_exchange(partial_value, "chan"), axis=0)
    delta_all = jax.nn.softplus(
        lax.dot_general(
            dbc[:, :RANK].astype(jnp.bfloat16),
            dt_proj_w,
            contract_last,
            preferred_element_type=jnp.float32,
        )
        + dt_bias
    ).reshape(steps, rows, -1)
    dbc = dbc.reshape(steps, rows, -1)
    state = ssm_state
    sums = []
    for step in range(steps):
        b_mat = dbc[step, :, RANK : RANK + NSTATE]
        c_mat = dbc[step, :, RANK + NSTATE :]
        delta = delta_all[step]
        act_real = acts[step].astype(jnp.float32)
        state = (
            jnp.exp(delta[:, None, :] * decay[None]) * state
            + (delta * act_real)[:, None, :] * b_mat[:, :, None]
        )
        sums.append(jnp.sum(c_mat[:, :, None] * state, axis=1) + d_skip * act_real)
    y_all = jnp.concatenate(sums, axis=0)
    z_in = jnp.dot(normed, relay_z, preferred_element_type=jnp.float32).astype(jnp.bfloat16)
    gated = (y_all * jax.nn.silu(z_in.astype(jnp.float32))).astype(jnp.bfloat16)
    mixed = []
    for part in relay_out:
        terms = jnp.stack(
            [
                lax.dot_general(
                    gated, block, contract_last, preferred_element_type=jnp.float32
                ).astype(jnp.bfloat16)
                for block in part.reshape(groups, -1, part.shape[1])
            ]
        )
        landed = exchange(terms, "chan")
        mixed.append(jnp.sum(landed.astype(jnp.float32), axis=0))
    blocks = [m.reshape(steps * rows, replicas // groups, half) for m in mixed]
    mixed_all = jnp.stack(blocks, axis=2).reshape(steps * rows, -1)
    block_out = (found.astype(jnp.float32) + mixed_all).astype(jnp.bfloat16)
    window_state = jnp.transpose(window[steps:], (1, 0, 2))
    return (in_new, out_new, block_out.reshape(steps, rows, -1), window_state, state)


def solution(mesh):
    placed = (
        P(("fsdp", "chan"), None, None),
        P(("fsdp", "chan"), None, None),
        P(("fsdp", "chan"), None, None),
        P(("fsdp", "chan"), None, None),
        P(("fsdp", "chan"), None),
        P(("fsdp", "chan"), None),
        P(("fsdp", "chan"), None),
        P(("fsdp", "chan"), None),
        P("fsdp", "chan"),
        P(None, "fsdp"),
        P("fsdp", None, "chan"),
        P("fsdp", None, "chan"),
        P(None, "chan"),
        P("chan"),
        P(None, "chan"),
        P("chan", None),
        P("chan"),
        P(None, "chan"),
        P("chan"),
    )
    return jax.shard_map(
        per_device,
        mesh=mesh,
        in_specs=placed,
        out_specs=(
            P(("fsdp", "chan"), None, None),
            P(("fsdp", "chan"), None),
            P(None, "fsdp", "chan"),
            P("fsdp", None, "chan"),
            P("fsdp", None, "chan"),
        ),
        check_vma=False,
    )
```

```python
import math

import jax
import jax.numpy as jnp
from jax import lax
from jax.experimental.layout import Layout, with_layout_constraint
from jax.sharding import PartitionSpec as P

RANK = 256
NSTATE = 16


learn_rate = 0.01
beta_first = 0.8
beta_second = 0.95
adam_eps = 1e-08
weight_decay = 0.1
bias_first = 1.0 - math.pow(0.8, 10)
bias_second = 1.0 - math.pow(0.95, 10)
norm_eps = 1e-06


def adam_update(master, moment, velocity, grad):
    gradient = grad.astype(jnp.float32)
    moment = beta_first * moment + (1.0 - beta_first) * gradient
    velocity = beta_second * velocity + (1.0 - beta_second) * gradient * gradient
    update = moment / bias_first / (jnp.sqrt(velocity / bias_second) + adam_eps)
    return master - learn_rate * (update + weight_decay * master)


def row_major(block):
    return with_layout_constraint(block, Layout(tuple(range(block.ndim))))


def exchange(block, axis):
    return row_major(
        lax.all_to_all(row_major(block), axis, split_axis=0, concat_axis=0, tiled=True)
    )


def gather_by_exchange(block, axis):
    count = lax.axis_size(axis)
    spread = jnp.broadcast_to(block[None], (count,) + block.shape)
    return exchange(spread, axis)


def owned_rank(member):
    length = member.shape[0]
    earlier = lax.broadcasted_iota(jnp.int32, (length, length), 1) < lax.broadcasted_iota(
        jnp.int32, (length, length), 0
    )
    return jnp.dot(
        earlier.astype(jnp.bfloat16),
        member.astype(jnp.bfloat16),
        preferred_element_type=jnp.float32,
    ).astype(jnp.int32)


def pick_rows(embed_table, tokens):
    replicas = lax.axis_size("fsdp")
    vocab_rows = embed_table.shape[0]
    mine = tokens.reshape(-1)
    count = mine.shape[0]
    cap = 2 * count // replicas
    every = lax.all_gather(mine, "fsdp", axis=0, tiled=False)
    offset = every - lax.axis_index("fsdp") * vocab_rows
    inside = jnp.logical_and(offset >= 0, offset < vocab_rows)
    rank = owned_rank(inside.T).T
    key = jnp.where(inside, rank, -1)
    slot_ids = lax.broadcasted_iota(jnp.int32, (replicas, cap, count), 1)
    slots = jnp.sum(jnp.where(key[:, None, :] == slot_ids, offset[:, None, :], 0), axis=2)
    return embed_table.at[slots.reshape(-1)].get(mode="clip")


def find_inputs(embed_table, tokens, got):
    replicas = lax.axis_size("fsdp")
    vocab_rows = embed_table.shape[0]
    mine = tokens.reshape(-1)
    count = mine.shape[0]
    cap = 2 * count // replicas
    owner = mine // vocab_rows
    member = owner[:, None] == lax.broadcasted_iota(jnp.int32, (count, replicas), 1)
    place = owner * cap + jnp.sum(jnp.where(member, owned_rank(member), 0), axis=1)
    pick = place[:, None] == lax.broadcasted_iota(jnp.int32, (count, replicas * cap), 1)
    return jnp.dot(pick.astype(jnp.bfloat16), got, preferred_element_type=jnp.float32).astype(
        jnp.bfloat16
    )


def per_device(
    in_master,
    in_moment,
    in_velocity,
    in_grad,
    out_master,
    out_moment,
    out_velocity,
    out_grad,
    embed_table,
    tokens,
    conv_state,
    ssm_state,
    conv_weight,
    conv_bias,
    x_proj_w,
    dt_proj_w,
    dt_bias,
    a_log,
    d_skip,
):
    groups = lax.axis_size("chan")
    replicas = lax.axis_size("fsdp")
    steps, rows = tokens.shape
    out_new = adam_update(out_master, out_moment, out_velocity, out_grad)
    out_new = lax.optimization_barrier(row_major(out_new))

    def split_columns(piece):
        wide = piece.shape[1] // groups
        cuts = [piece[:, at * wide : (at + 1) * wide] for at in range(groups)]
        return row_major(jnp.stack(cuts).astype(jnp.bfloat16))

    def to_groups(split):
        return exchange(split, "chan").reshape(-1, split.shape[2])

    out_split = lax.optimization_barrier(split_columns(out_new))
    out_own = to_groups(out_split)
    tokens, out_own = lax.optimization_barrier((tokens, out_own))
    rows_found = pick_rows(embed_table, tokens)
    in_master, in_grad, rows_found = lax.optimization_barrier((in_master, in_grad, rows_found))
    in_new = adam_update(in_master, in_moment, in_velocity, in_grad)
    in_new = lax.optimization_barrier(row_major(in_new))
    x_split = split_columns(in_new[:, 0, :])
    z_split = split_columns(in_new[:, 1, :])
    got = exchange(rows_found, "fsdp")
    x_split, z_split, got = lax.optimization_barrier((x_split, z_split, got))
    x_own = to_groups(x_split)
    z_split, x_own = lax.optimization_barrier((z_split, x_own))
    z_own = to_groups(z_split)
    got, x_own, z_own = lax.optimization_barrier((got, x_own, z_own))
    half = out_own.shape[0] // 2
    relay_first = lax.all_gather(out_own[:half], "fsdp", axis=0, tiled=True)
    x_own, z_own, relay_first = lax.optimization_barrier((x_own, z_own, relay_first))
    relay_x = lax.all_gather(x_own, "fsdp", axis=0, tiled=True)
    relay_z = lax.all_gather(z_own, "fsdp", axis=0, tiled=True)
    out_rest, relay_x = lax.optimization_barrier((out_own[half:], relay_x))
    relay_out = [relay_first, lax.all_gather(out_rest, "fsdp", axis=0, tiled=True)]

    found = find_inputs(embed_table, tokens, got)
    parts = gather_by_exchange(found, "chan")
    flat = parts.astype(jnp.float32)
    width = groups * parts.shape[2]
    square = jnp.sum(jnp.sum(flat * flat, axis=2), axis=0) / width
    scale = lax.rsqrt(square + norm_eps)
    normed = (flat * scale[None, :, None]).astype(jnp.bfloat16)
    normed = jnp.transpose(normed, (1, 0, 2)).reshape(steps * rows, width)
    x_in = (
        jnp.dot(normed, relay_x, preferred_element_type=jnp.float32)
        .astype(jnp.bfloat16)
        .reshape(steps, rows, -1)
    )
    decay = -jnp.exp(a_log)
    contract_last = (((1,), (1,)), ((), ()))
    window = jnp.concatenate([jnp.transpose(conv_state, (1, 0, 2)), x_in], axis=0)
    taps = conv_weight.shape[0]
    acts = []
    for step in range(steps):
        total = conv_bias
        for tap in range(taps):
            total = total + window[step + tap].astype(jnp.float32) * conv_weight[tap]
        acts.append(jax.nn.silu(total).astype(jnp.bfloat16))
    act_all = jnp.concatenate(acts, axis=0)
    partial_value = lax.dot_general(
        act_all, x_proj_w, contract_last, preferred_element_type=jnp.float32
    )
    dbc = jnp.sum(gather_by_exchange(partial_value, "chan"), axis=0)
    delta_all = jax.nn.softplus(
        lax.dot_general(
            dbc[:, :RANK].astype(jnp.bfloat16),
            dt_proj_w,
            contract_last,
            preferred_element_type=jnp.float32,
        )
        + dt_bias
    ).reshape(steps, rows, -1)
    dbc = dbc.reshape(steps, rows, -1)
    state = ssm_state
    sums = []
    for step in range(steps):
        b_mat = dbc[step, :, RANK : RANK + NSTATE]
        c_mat = dbc[step, :, RANK + NSTATE :]
        delta = delta_all[step]
        act_real = acts[step].astype(jnp.float32)
        state = (
            jnp.exp(delta[:, None, :] * decay[None]) * state
            + (delta * act_real)[:, None, :] * b_mat[:, :, None]
        )
        sums.append(jnp.sum(c_mat[:, :, None] * state, axis=1) + d_skip * act_real)
    y_all = jnp.concatenate(sums, axis=0)
    z_in = jnp.dot(normed, relay_z, preferred_element_type=jnp.float32).astype(jnp.bfloat16)
    gated = (y_all * jax.nn.silu(z_in.astype(jnp.float32))).astype(jnp.bfloat16)
    mixed = []
    for part in relay_out:
        terms = jnp.stack(
            [
                lax.dot_general(
                    gated, block, contract_last, preferred_element_type=jnp.float32
                ).astype(jnp.bfloat16)
                for block in part.reshape(groups, -1, part.shape[1])
            ]
        )
        landed = exchange(terms, "chan")
        mixed.append(jnp.sum(landed.astype(jnp.float32), axis=0))
    cuts = [
        m[:, at * half : (at + 1) * half] for at in range(replicas // groups) for m in mixed
    ]
    mixed_all = jnp.concatenate(cuts, axis=1)
    block_out = (found.astype(jnp.float32) + mixed_all).astype(jnp.bfloat16)
    window_state = jnp.transpose(window[steps:], (1, 0, 2))
    return (in_new, out_new, block_out.reshape(steps, rows, -1), window_state, state)


def solution(mesh):
    placed = (
        P(("fsdp", "chan"), None, None),
        P(("fsdp", "chan"), None, None),
        P(("fsdp", "chan"), None, None),
        P(("fsdp", "chan"), None, None),
        P(("fsdp", "chan"), None),
        P(("fsdp", "chan"), None),
        P(("fsdp", "chan"), None),
        P(("fsdp", "chan"), None),
        P("fsdp", "chan"),
        P(None, "fsdp"),
        P("fsdp", None, "chan"),
        P("fsdp", None, "chan"),
        P(None, "chan"),
        P("chan"),
        P(None, "chan"),
        P("chan", None),
        P("chan"),
        P(None, "chan"),
        P("chan"),
    )
    return jax.shard_map(
        per_device,
        mesh=mesh,
        in_specs=placed,
        out_specs=(
            P(("fsdp", "chan"), None, None),
            P(("fsdp", "chan"), None),
            P(None, "fsdp", "chan"),
            P("fsdp", None, "chan"),
            P("fsdp", None, "chan"),
        ),
        check_vma=False,
    )
```

```python
import math

import jax
import jax.numpy as jnp
from jax import lax
from jax.experimental.layout import Layout, with_layout_constraint
from jax.sharding import PartitionSpec as P

RANK = 256
NSTATE = 16


learn_rate = 0.01
beta_first = 0.8
beta_second = 0.95
adam_eps = 1e-08
weight_decay = 0.1
bias_first = 1.0 - math.pow(0.8, 10)
bias_second = 1.0 - math.pow(0.95, 10)
norm_eps = 1e-06


def adam_update(master, moment, velocity, grad):
    gradient = grad.astype(jnp.float32)
    moment = beta_first * moment + (1.0 - beta_first) * gradient
    velocity = beta_second * velocity + (1.0 - beta_second) * gradient * gradient
    update = moment / bias_first / (jnp.sqrt(velocity / bias_second) + adam_eps)
    return master - learn_rate * (update + weight_decay * master)


def row_major(block):
    return with_layout_constraint(block, Layout(tuple(range(block.ndim))))


def exchange(block, axis):
    return row_major(
        lax.all_to_all(row_major(block), axis, split_axis=0, concat_axis=0, tiled=True)
    )


def gather_by_exchange(block, axis):
    count = lax.axis_size(axis)
    spread = jnp.broadcast_to(block[None], (count,) + block.shape)
    return exchange(spread, axis)


def owned_rank(member):
    length = member.shape[0]
    earlier = lax.broadcasted_iota(jnp.int32, (length, length), 1) < lax.broadcasted_iota(
        jnp.int32, (length, length), 0
    )
    return jnp.dot(
        earlier.astype(jnp.bfloat16),
        member.astype(jnp.bfloat16),
        preferred_element_type=jnp.float32,
    ).astype(jnp.int32)


def pick_rows(embed_table, tokens):
    replicas = lax.axis_size("fsdp")
    vocab_rows = embed_table.shape[0]
    mine = tokens.reshape(-1)
    count = mine.shape[0]
    cap = 2 * count // replicas
    every = lax.all_gather(mine, "fsdp", axis=0, tiled=False)
    offset = every - lax.axis_index("fsdp") * vocab_rows
    inside = jnp.logical_and(offset >= 0, offset < vocab_rows)
    rank = owned_rank(inside.T).T
    key = jnp.where(inside, rank, -1)
    slot_ids = lax.broadcasted_iota(jnp.int32, (replicas, cap, count), 1)
    slots = jnp.sum(jnp.where(key[:, None, :] == slot_ids, offset[:, None, :], 0), axis=2)
    return embed_table.at[slots.reshape(-1)].get(mode="clip")


def find_inputs(embed_table, tokens, got):
    replicas = lax.axis_size("fsdp")
    vocab_rows = embed_table.shape[0]
    mine = tokens.reshape(-1)
    count = mine.shape[0]
    cap = 2 * count // replicas
    owner = mine // vocab_rows
    member = owner[:, None] == lax.broadcasted_iota(jnp.int32, (count, replicas), 1)
    place = owner * cap + jnp.sum(jnp.where(member, owned_rank(member), 0), axis=1)
    pick = place[:, None] == lax.broadcasted_iota(jnp.int32, (count, replicas * cap), 1)
    return jnp.dot(pick.astype(jnp.bfloat16), got, preferred_element_type=jnp.float32).astype(
        jnp.bfloat16
    )


def per_device(
    in_master,
    in_moment,
    in_velocity,
    in_grad,
    out_master,
    out_moment,
    out_velocity,
    out_grad,
    embed_table,
    tokens,
    conv_state,
    ssm_state,
    conv_weight,
    conv_bias,
    x_proj_w,
    dt_proj_w,
    dt_bias,
    a_log,
    d_skip,
):
    groups = lax.axis_size("chan")
    replicas = lax.axis_size("fsdp")
    steps, rows = tokens.shape
    out_new = adam_update(out_master, out_moment, out_velocity, out_grad)
    out_new = lax.optimization_barrier(row_major(out_new))

    def split_columns(piece):
        wide = piece.shape[1] // groups
        cuts = [piece[:, at * wide : (at + 1) * wide] for at in range(groups)]
        return row_major(jnp.stack(cuts).astype(jnp.bfloat16))

    def to_groups(split):
        return exchange(split, "chan").reshape(-1, split.shape[2])

    out_split = lax.optimization_barrier(split_columns(out_new))
    out_own = to_groups(out_split)
    tokens, out_own = lax.optimization_barrier((tokens, out_own))
    rows_found = pick_rows(embed_table, tokens)
    in_master, in_grad, rows_found = lax.optimization_barrier((in_master, in_grad, rows_found))
    in_new = adam_update(in_master, in_moment, in_velocity, in_grad)
    in_new = lax.optimization_barrier(row_major(in_new))
    x_split = split_columns(in_new[:, 0, :])
    z_split = split_columns(in_new[:, 1, :])
    got = exchange(rows_found, "fsdp")
    x_own = to_groups(x_split)
    half = out_own.shape[0] // 2
    relay_first = lax.all_gather(out_own[:half], "fsdp", axis=0, tiled=True)
    z_split, relay_first, x_own = lax.optimization_barrier((z_split, relay_first, x_own))
    relay_x = lax.all_gather(x_own, "fsdp", axis=0, tiled=True)
    z_own = to_groups(z_split)
    got, z_own = lax.optimization_barrier((got, z_own))
    relay_z = lax.all_gather(z_own, "fsdp", axis=0, tiled=True)
    out_rest, relay_x = lax.optimization_barrier((out_own[half:], relay_x))
    relay_out = [relay_first, lax.all_gather(out_rest, "fsdp", axis=0, tiled=True)]

    found = find_inputs(embed_table, tokens, got)
    parts = gather_by_exchange(found, "chan")
    flat = parts.astype(jnp.float32)
    width = groups * parts.shape[2]
    square = jnp.sum(jnp.sum(flat * flat, axis=2), axis=0) / width
    scale = lax.rsqrt(square + norm_eps)
    normed = (flat * scale[None, :, None]).astype(jnp.bfloat16)
    normed = jnp.transpose(normed, (1, 0, 2)).reshape(steps * rows, width)
    x_in = (
        jnp.dot(normed, relay_x, preferred_element_type=jnp.float32)
        .astype(jnp.bfloat16)
        .reshape(steps, rows, -1)
    )
    decay = -jnp.exp(a_log)
    contract_last = (((1,), (1,)), ((), ()))
    window = jnp.concatenate([jnp.transpose(conv_state, (1, 0, 2)), x_in], axis=0)
    taps = conv_weight.shape[0]
    acts = []
    for step in range(steps):
        total = conv_bias
        for tap in range(taps):
            total = total + window[step + tap].astype(jnp.float32) * conv_weight[tap]
        acts.append(jax.nn.silu(total).astype(jnp.bfloat16))
    act_all = jnp.concatenate(acts, axis=0)
    partial_value = lax.dot_general(
        act_all, x_proj_w, contract_last, preferred_element_type=jnp.float32
    )
    dbc = jnp.sum(gather_by_exchange(partial_value, "chan"), axis=0)
    delta_all = jax.nn.softplus(
        lax.dot_general(
            dbc[:, :RANK].astype(jnp.bfloat16),
            dt_proj_w,
            contract_last,
            preferred_element_type=jnp.float32,
        )
        + dt_bias
    ).reshape(steps, rows, -1)
    dbc = dbc.reshape(steps, rows, -1)
    state = ssm_state
    sums = []
    for step in range(steps):
        b_mat = dbc[step, :, RANK : RANK + NSTATE]
        c_mat = dbc[step, :, RANK + NSTATE :]
        delta = delta_all[step]
        act_real = acts[step].astype(jnp.float32)
        state = (
            jnp.exp(delta[:, None, :] * decay[None]) * state
            + (delta * act_real)[:, None, :] * b_mat[:, :, None]
        )
        sums.append(jnp.sum(c_mat[:, :, None] * state, axis=1) + d_skip * act_real)
    y_all = jnp.concatenate(sums, axis=0)
    z_in = jnp.dot(normed, relay_z, preferred_element_type=jnp.float32).astype(jnp.bfloat16)
    gated = (y_all * jax.nn.silu(z_in.astype(jnp.float32))).astype(jnp.bfloat16)
    mixed = []
    for part in relay_out:
        terms = jnp.stack(
            [
                lax.dot_general(
                    gated, block, contract_last, preferred_element_type=jnp.float32
                ).astype(jnp.bfloat16)
                for block in part.reshape(groups, -1, part.shape[1])
            ]
        )
        landed = exchange(terms, "chan")
        mixed.append(jnp.sum(landed.astype(jnp.float32), axis=0))
    cuts = [
        m[:, at * half : (at + 1) * half] for at in range(replicas // groups) for m in mixed
    ]
    mixed_all = jnp.concatenate(cuts, axis=1)
    block_out = (found.astype(jnp.float32) + mixed_all).astype(jnp.bfloat16)
    window_state = jnp.transpose(window[steps:], (1, 0, 2))
    return (in_new, out_new, block_out.reshape(steps, rows, -1), window_state, state)


def solution(mesh):
    placed = (
        P(("fsdp", "chan"), None, None),
        P(("fsdp", "chan"), None, None),
        P(("fsdp", "chan"), None, None),
        P(("fsdp", "chan"), None, None),
        P(("fsdp", "chan"), None),
        P(("fsdp", "chan"), None),
        P(("fsdp", "chan"), None),
        P(("fsdp", "chan"), None),
        P("fsdp", "chan"),
        P(None, "fsdp"),
        P("fsdp", None, "chan"),
        P("fsdp", None, "chan"),
        P(None, "chan"),
        P("chan"),
        P(None, "chan"),
        P("chan", None),
        P("chan"),
        P(None, "chan"),
        P("chan"),
    )
    return jax.shard_map(
        per_device,
        mesh=mesh,
        in_specs=placed,
        out_specs=(
            P(("fsdp", "chan"), None, None),
            P(("fsdp", "chan"), None),
            P(None, "fsdp", "chan"),
            P("fsdp", None, "chan"),
            P("fsdp", None, "chan"),
        ),
        check_vma=False,
    )
```
